32 devices in a mesh: node: 4 (over x, core), space: 8 (over z, y).
Axes of the slice: x: 2, y: 2, z: 4, core: 2. Of those that a mesh axis runs over, the one named last changes fastest.
Arguments:
- initial: float32 [32, 256, 256], P('space'), may hold values from -1 to 1
- kappa: float32 [32, 256, 256], P('space'), may hold values from 0.3 to 3
Outputs:
- sections: float32 [4, 32, 256, 256], P('node', 'space')
The draws below stay inside these ranges and needn't reach their ends.
All inputs are finite; a program needn't handle non-finite values.
Results may differ from the reference program's by a relative error of at most 0.0002.
Values sent between devices are 32-bit elements; how exact they have to be, the bound alone decides.
A program may use at most 192 MiB of HBM per device.

```python
import math
import jax
import jax.numpy as jnp
from jax import lax

M = 4
NXY = 256
NZ = 32
SWEEPS = 2
VCYCLES = 2
SMOOTH = 2
LEVELS = 3
COARSE = 8


def level_of(own_key, shape, cuts, low, largest):
    gain = 1.0
    for axis_at, shards_of in cuts:
        heights = jax.random.uniform(jax.random.fold_in(jax.random.fold_in(own_key, 6), axis_at), (shards_of,), jnp.float32, low / len(cuts), largest / len(cuts))
        gain = gain * jnp.repeat(jnp.exp(heights), shape[axis_at] // shards_of).reshape((-1,) + (1,) * (len(shape) - 1 - axis_at))
    return gain


def setup_inputs(seed: int = 0) -> dict:
    splits = jax.random.split(jax.random.key(seed), 3)
    initial = jnp.clip(jax.random.uniform(splits[0], (NZ, NXY, NXY), jnp.float32, -1.0, 1.0) * level_of(splits[0], (NZ, NXY, NXY), ((0, 8),), -0.4, 0.0), -1.0, 1.0)
    kappa = jnp.clip(jnp.exp(math.log(3.0) - 2.3025851 * jax.random.uniform(splits[1], (NZ, NXY, NXY), jnp.float32) ** level_of(splits[1], (NZ, NXY, NXY), ((0, 8),), -0.2, 0.2)), 0.3, 3.0)
    return {"initial": initial, "kappa": kappa}


DIFFUSE = 2.0
REACT = 0.5
OMEGA = 0.8


def radau_gap(count, where):
    previous = 1.0
    current = where
    for degree in range(1, count):
        following = ((2 * degree + 1) * where * current - degree * previous) / (degree + 1)
        previous = current
        current = following
    return current - previous


def radau_table(count):
    zeros_found = []
    grid_count = 4096
    lower = -1.0
    value_low = radau_gap(count, lower)
    for place in range(1, grid_count):
        upper = -1.0 + 2.0 * place / grid_count
        value_up = radau_gap(count, upper)
        if value_low * value_up < 0.0:
            left_end = lower
            right_end = upper
            left_value = value_low
            for halving in range(100):
                middle = 0.5 * (left_end + right_end)
                middle_value = radau_gap(count, middle)
                if left_value * middle_value <= 0.0:
                    right_end = middle
                else:
                    left_end = middle
                    left_value = middle_value
            zeros_found.append(0.5 * (left_end + right_end))
        lower = upper
        value_low = value_up
    zeros_found.append(1.0)
    abscissa = [(value + 1.0) / 2.0 for value in zeros_found]
    table_rows = []
    for outer in range(count):
        table_rows.append([0.0] * count)
    for column in range(count):
        factor = [1.0]
        scale = 1.0
        for other in range(count):
            if other != column:
                widened = [0.0] * (len(factor) + 1)
                for power in range(len(factor)):
                    widened[power + 1] = widened[power + 1] + factor[power]
                    widened[power] = widened[power] - abscissa[other] * factor[power]
                factor = widened
                scale = scale * (abscissa[column] - abscissa[other])
        for outer in range(count):
            upto = abscissa[outer]
            accum = 0.0
            for power in range(len(factor)):
                accum = accum + factor[power] * upto ** (power + 1) / (power + 1)
            table_rows[outer][column] = accum / scale
    return abscissa, table_rows


def laplace(field):
    total = jnp.roll(field, -1, 1) + jnp.roll(field, 1, 1)
    total = total + jnp.roll(field, 1, 2) + jnp.roll(field, -1, 2)
    total = total + jnp.roll(field, 1, 3) + jnp.roll(field, -1, 3)
    return total - 6.0 * field


def smooth(field, source, shift):
    applied = field - shift * laplace(field)
    return field + OMEGA * (source - applied) / (1.0 + 6.0 * shift)


def restrict(field):
    a, b, c, d = field.shape
    return field.reshape(a, b // 2, 2, c // 2, 2, d // 2, 2).mean(axis=(2, 4, 6))


def prolong(field):
    return jnp.repeat(jnp.repeat(jnp.repeat(field, 2, 1), 2, 2), 2, 3)


def vcycle(level, field, source, shift):
    if level == LEVELS - 1:
        field = jnp.zeros_like(source)
        for sweep in range(COARSE):
            field = smooth(field, source, shift)
        return field
    if field is None:
        field = jnp.zeros_like(source)
    for sweep in range(SMOOTH):
        field = smooth(field, source, shift)
    remain = source - (field - shift * laplace(field))
    coarse_part = vcycle(level + 1, None, restrict(remain), shift / 4.0)
    field = field + prolong(coarse_part)
    for sweep in range(SMOOTH):
        field = smooth(field, source, shift)
    return field


def reference(initial, kappa):
    abscissa, table_rows = radau_table(M)
    quadrature = jnp.asarray(table_rows, jnp.float32)
    shift = jnp.asarray([DIFFUSE * value for value in abscissa], jnp.float32).reshape(M, 1, 1, 1)
    sections = jnp.broadcast_to(initial, (M,) + initial.shape).astype(jnp.float32)
    for sweep in range(SWEEPS):
        lap = laplace(sections)
        force = DIFFUSE * lap + REACT * kappa * (sections - sections * sections * sections)
        integral = jnp.einsum("mj,jzyx->mzyx", quadrature, force, precision=lax.Precision.HIGHEST)
        right = initial + integral - shift * lap
        for cycle in range(VCYCLES):
            sections = vcycle(0, sections, right, shift)
    return sections
```

```python
import functools

import jax
import jax.numpy as jnp
from jax import lax
from jax.experimental import pallas as pl
from jax.experimental.pallas import tpu as pltpu
from jax.sharding import PartitionSpec as P

SWEEPS = 2
VCYCLES = 2
COARSE = 8

DIFFUSE = 2.0
REACT = 0.5
OMEGA = 0.8

HALO = 4
EXACT = lax.Precision.HIGHEST


def radau_gap(count, where):
    previous = 1.0
    current = where
    for degree in range(1, count):
        following = ((2 * degree + 1) * where * current - degree * previous) / (degree + 1)
        previous = current
        current = following
    return current - previous


def radau_table(count):
    zeros_found = []
    grid_count = 4096
    lower = -1.0
    value_low = radau_gap(count, lower)
    for place in range(1, grid_count):
        upper = -1.0 + 2.0 * place / grid_count
        value_up = radau_gap(count, upper)
        if value_low * value_up < 0.0:
            left_end = lower
            right_end = upper
            left_value = value_low
            for halving in range(100):
                middle = 0.5 * (left_end + right_end)
                middle_value = radau_gap(count, middle)
                if left_value * middle_value <= 0.0:
                    right_end = middle
                else:
                    left_end = middle
                    left_value = middle_value
            zeros_found.append(0.5 * (left_end + right_end))
        lower = upper
        value_low = value_up
    zeros_found.append(1.0)
    abscissa = [(value + 1.0) / 2.0 for value in zeros_found]
    table_rows = []
    for outer in range(count):
        table_rows.append([0.0] * count)
    for column in range(count):
        factor = [1.0]
        scale = 1.0
        for other in range(count):
            if other != column:
                widened = [0.0] * (len(factor) + 1)
                for power in range(len(factor)):
                    widened[power + 1] = widened[power + 1] + factor[power]
                    widened[power] = widened[power] - abscissa[other] * factor[power]
                factor = widened
                scale = scale * (abscissa[column] - abscissa[other])
        for outer in range(count):
            upto = abscissa[outer]
            accum = 0.0
            for power in range(len(factor)):
                accum = accum + factor[power] * upto ** (power + 1) / (power + 1)
            table_rows[outer][column] = accum / scale
    return (abscissa, table_rows)


def ring_order(count):
    return list(range(0, count, 2)) + list(range(count - 1 - count % 2, 0, -2))


def rows_loop(count, body):
    step = next(k for k in (4, 3, 2, 1) if count % k == 0)

    def some(i, carry):
        for k in range(step):
            body(i * step + k)
        return carry

    lax.fori_loop(0, count // step, some, 0)


def six(ref, row):
    here = ref[row]
    tall, wide = here.shape
    total = ref[row - 1] + ref[row + 1]
    total = total + (pltpu.roll(here, 1, 0) + pltpu.roll(here, tall - 1, 0))
    total = total + (pltpu.roll(here, 1, 1) + pltpu.roll(here, wide - 1, 1))
    return here, total


def sweep(src, src_at, source, source_at, dst, dst_at, count, shift):
    weight = OMEGA / (1.0 + 6.0 * shift)
    spread = weight * shift

    def body(row):
        here, total = six(src, row + src_at)
        dst[row + dst_at] = (1.0 - OMEGA) * here + weight * source[row + source_at] + spread * total

    rows_loop(count, body)


def residual(src, src_at, source, source_at, row, shift):
    here, total = six(src, row + src_at)
    return source[row + source_at] - (1.0 + 6.0 * shift) * here + shift * total


def copy_rows(src, src_at, dst, dst_at, count):
    def body(row):
        dst[row + dst_at] = src[row + src_at]

    rows_loop(count, body)


def force_kernel(shift_ref, lo, mid, hi, first, kappa, force, base, wide):
    shift = shift_ref[0]
    count = mid.shape[0]
    copy_rows(lo, 0, wide, 0, HALO)
    copy_rows(mid, 0, wide, HALO, count)
    copy_rows(hi, 0, wide, HALO + count, HALO)

    def body(row):
        here, total = six(wide, row + 1)
        lap = total - 6.0 * here
        strength = kappa[row + 1]
        force[row] = DIFFUSE * lap + REACT * strength * (here - here * here * here)
        base[row] = first[row + 1] - shift * lap

    rows_loop(count + 2 * HALO - 2, body)


def before_kernel(shift_ref, lo, mid, hi, right, squeeze, field, source1, wide, other, summed, thin):
    shift = shift_ref[0]
    count = mid.shape[0]
    copy_rows(lo, 0, wide, 0, HALO)
    copy_rows(mid, 0, wide, HALO, count)
    copy_rows(hi, 0, wide, HALO + count, HALO)
    sweep(wide, 1, right, 0, other, 0, count + 6, shift)
    sweep(other, 1, right, 1, field, 0, count + 4, shift)

    def body(row):
        at = 2 * row
        summed[row] = residual(field, at + 2, right, at + 3, 0, shift) + residual(
            field, at + 3, right, at + 4, 0, shift
        )

    rows_loop(count // 2, body)
    half, tall, across = summed.shape
    thin[...] = jnp.dot(summed[...].reshape(half * tall, across), squeeze[...], precision=EXACT).reshape(thin.shape)
    source1[...] = thin[:, pl.ds(0, tall // 2, stride=2), :] + thin[:, pl.ds(1, tall // 2, stride=2), :]


def middle_kernel(shift_ref, lo, mid, hi, squeeze, field1, wide1, source2, first, summed):
    shift = shift_ref[0] / 4.0
    count = mid.shape[0]
    copy_rows(lo, 0, wide1, 0, HALO)
    copy_rows(mid, 0, wide1, HALO, count)
    copy_rows(hi, 0, wide1, HALO + count, HALO)
    weight = OMEGA / (1.0 + 6.0 * shift)

    def start(row):
        first[row] = weight * wide1[row]

    rows_loop(count + 2 * HALO, start)
    sweep(first, 1, wide1, 1, field1, 0, count + 6, shift)

    def body(row):
        at = 2 * row
        summed[row] = residual(field1, at + 3, wide1, at + 4, 0, shift) + residual(
            field1, at + 4, wide1, at + 5, 0, shift
        )

    rows_loop(count // 2, body)
    half, tall, across = summed.shape
    short = summed[:, pl.ds(0, tall // 2, stride=2), :] + summed[:, pl.ds(1, tall // 2, stride=2), :]
    short = short.reshape(half * tall // 2, across)
    source2[...] = jnp.dot(short, squeeze[...], precision=EXACT).reshape(source2.shape)


def after_kernel(
    order, shift_ref, place, parts, field1, wide1, field, right, stretch2, stretch1, out,
    source2, even, odd, error2, work1, more1, error1, work, more, last,
):
    shift = shift_ref[0]
    shift1 = shift / 4.0
    shift2 = shift1 / 4.0
    devices, own = parts.shape[:2]
    rows = devices * own
    for at, device in enumerate(order):
        source2[pl.ds(at * own, own)] = parts[device]
    weight = OMEGA / (1.0 + 6.0 * shift2)

    def start(row):
        even[row + 1] = weight * source2[row]

    rows_loop(rows, start)
    here, there = even, odd
    for step in range(COARSE - 1):
        here[0] = here[rows]
        here[rows + 1] = here[1]
        sweep(here, 1, source2, 0, there, 1, rows, shift2)
        here, there = there, here
    begin = place[0] * own

    def pick(row):
        error2[row] = here[lax.rem(begin + row - 2 + rows, rows) + 1]

    rows_loop(own + 4, pick)
    tall2 = error2.shape[1]
    spread = jnp.dot(
        error2[...].reshape((own + 4) * tall2, error2.shape[2]), stretch2[...], precision=EXACT
    ).reshape(own + 4, tall2, stretch2.shape[1])
    tall1 = 2 * tall2
    work1[:, pl.ds(0, tall2, stride=2), :] = spread
    work1[:, pl.ds(1, tall2, stride=2), :] = spread
    count1 = 2 * own

    def correct1(row):
        more1[row] = field1[row] + work1[(row + 1) // 2]

    rows_loop(count1 + 6, correct1)
    sweep(more1, 1, wide1, 2, error1, 0, count1 + 4, shift1)
    sweep(error1, 1, wide1, 3, more1, 0, count1 + 2, shift1)
    tall = 2 * tall1
    half = more1[pl.ds(0, count1 + 2)]
    work[:, pl.ds(0, tall1, stride=2), :] = half
    work[:, pl.ds(1, tall1, stride=2), :] = half
    count = 2 * count1

    def correct(row):
        fine = jnp.dot(work[row], stretch1[...], precision=EXACT)
        more[2 * row] = field[2 * row] + fine
        more[2 * row + 1] = field[2 * row + 1] + fine

    rows_loop(count1 + 2, correct)
    sweep(more, 1, right, 2, last, 0, count + 2, shift)
    sweep(last, 1, right, 3, out, 0, count, shift)


def call(kernel, outs, scratch, *args):
    specs = [pl.BlockSpec(memory_space=pltpu.SMEM if a.ndim == 1 else pltpu.VMEM) for a in args]
    return pl.pallas_call(
        kernel,
        out_shape=[jax.ShapeDtypeStruct(shape, jnp.float32) for shape in outs],
        in_specs=specs,
        out_specs=[pl.BlockSpec(memory_space=pltpu.VMEM)] * len(outs),
        scratch_shapes=[pltpu.VMEM(shape, jnp.float32) for shape in scratch],
        compiler_params=pltpu.CompilerParams(vmem_limit_bytes=60 * 2**20),
    )(*args)


def pairing(fine, coarse, value):
    lanes = jnp.arange(coarse)[None, :] % (fine // 2)
    return jnp.where(jnp.arange(fine)[:, None] // 2 == lanes, value, 0.0).astype(jnp.float32)


def per_device(initial, kappa):
    nodes = lax.axis_size("node")
    position = lax.axis_index("node")
    devices = lax.axis_size("space")
    order = ring_order(devices)
    rank = [order.index(device) for device in range(devices)]
    place = jnp.asarray(rank, jnp.int32)[lax.axis_index("space")][None]
    up = [(order[i], order[(i + 1) % devices]) for i in range(devices)]
    down = [(target, source) for source, target in up]
    across = [(i, i ^ 1) for i in range(nodes)]
    abscissa, table_rows = radau_table(nodes)
    table = jnp.asarray(table_rows, jnp.float32)
    shift = jnp.asarray([DIFFUSE * value for value in abscissa], jnp.float32)[position]
    params = shift[None]

    planes, rows, cells = initial.shape
    tall = planes * devices
    own = rows // devices
    own1, tall1, cells1 = own // 2, tall // 2, cells // 2
    own2, tall2, cells2 = own // 4, tall // 4, max(128, cells // 4)
    squeeze = pairing(cells, cells1, 0.125)
    squeeze1 = pairing(cells1, cells2, 0.125)
    stretch1 = pairing(cells, cells1, 1.0).T
    stretch2 = jnp.where(jnp.arange(cells2)[None, :] < cells1 // 2, pairing(cells1, cells2, 1.0), 0.0).T

    def halo(mid):
        lo = lax.ppermute(mid[-HALO:], "space", up)
        hi = lax.ppermute(mid[:HALO], "space", down)
        return lo, mid, hi

    def spread_out(field):
        pieces = field.reshape(planes, devices, own, cells).transpose(1, 2, 0, 3)
        pieces = jnp.stack([pieces[at] for at in rank])
        pieces = lax.all_to_all(pieces, "space", 0, 0)
        return pieces.transpose(1, 0, 2, 3).reshape(own, tall, cells)

    def bring_back(field):
        pieces = field.reshape(own, devices, planes, cells).transpose(1, 2, 0, 3)
        pieces = lax.all_to_all(pieces, "space", 0, 0)
        pieces = jnp.stack([pieces[device] for device in order])
        return pieces.transpose(1, 0, 2, 3).reshape(planes, rows, cells)

    first_core = position % 2 == 0
    mine = jnp.concatenate(halo(spread_out(jnp.where(first_core, initial, kappa))))
    others = lax.ppermute(mine, "node", across)
    first = jnp.where(first_core, mine, others)
    strength = jnp.where(first_core, others, mine)
    parts = (first[:HALO], first[HALO:-HALO], first[-HALO:])

    extra = own + 2 * HALO
    for step in range(SWEEPS):
        force, base = call(
            force_kernel,
            [(extra - 2, tall, cells)] * 2,
            [(extra, tall, cells)],
            params, *parts, first, strength,
        )
        if step == 0:
            right = base + jnp.sum(table[position]) * force
        else:
            right = base
            held = force
            for turn in range(nodes // 2):
                if turn:
                    held = lax.ppermute(force, "node", [(i, (i + 2 * turn) % nodes) for i in range(nodes)])
                origin = (position - 2 * turn) % nodes
                beside = lax.ppermute(held, "node", across)
                right = right + table[position, origin] * held + table[position, origin ^ 1] * beside
        for cycle in range(VCYCLES):
            field, source1 = call(
                before_kernel,
                [(own + 4, tall, cells), (own1, tall1, cells1)],
                [(extra, tall, cells), (own + 6, tall, cells), (own1, tall, cells), (own1, tall, cells1)],
                params, *parts, right, squeeze,
            )
            field1, wide1, source2 = call(
                middle_kernel,
                [(own1 + 6, tall1, cells1), (own1 + 8, tall1, cells1), (own2, tall2, cells2)],
                [(own1 + 8, tall1, cells1), (own2, tall1, cells1)],
                params, *halo(source1), squeeze1,
            )
            pieces = lax.all_gather(source2, "space")
            (section,) = call(
                functools.partial(after_kernel, order),
                [(own, tall, cells)],
                [
                    (own2 * devices, tall2, cells2),
                    (own2 * devices + 2, tall2, cells2),
                    (own2 * devices + 2, tall2, cells2),
                    (own2 + 4, tall2, cells2),
                    (own2 + 4, tall1, cells1),
                    (own1 + 6, tall1, cells1),
                    (own1 + 4, tall1, cells1),
                    (own1 + 2, tall, cells1),
                    (own + 4, tall, cells),
                    (own + 2, tall, cells),
                ],
                params, place, pieces, field1, wide1, field, right, stretch2, stretch1,
            )
            if step + 1 < SWEEPS or cycle + 1 < VCYCLES:
                parts = halo(section)
    return bring_back(section)[None]


def solution(mesh):
    in_specs = (P("space", None, None), P("space", None, None))
    out_specs = P("node", "space", None, None)
    return jax.shard_map(
        per_device, mesh=mesh, in_specs=in_specs, out_specs=out_specs, check_vma=False
    )
```

```python
import functools

import jax
import jax.numpy as jnp
from jax import lax
from jax.experimental import pallas as pl
from jax.experimental.pallas import tpu as pltpu
from jax.sharding import PartitionSpec as P

SWEEPS = 2
VCYCLES = 2
COARSE = 8

DIFFUSE = 2.0
REACT = 0.5
OMEGA = 0.8

HALO = 4
MESH = pl.DeviceIdType.MESH


def radau_gap(count, where):
    previous = 1.0
    current = where
    for degree in range(1, count):
        following = ((2 * degree + 1) * where * current - degree * previous) / (degree + 1)
        previous = current
        current = following
    return current - previous


def radau_table(count):
    zeros_found = []
    grid_count = 4096
    lower = -1.0
    value_low = radau_gap(count, lower)
    for place in range(1, grid_count):
        upper = -1.0 + 2.0 * place / grid_count
        value_up = radau_gap(count, upper)
        if value_low * value_up < 0.0:
            left_end = lower
            right_end = upper
            left_value = value_low
            for halving in range(100):
                middle = 0.5 * (left_end + right_end)
                middle_value = radau_gap(count, middle)
                if left_value * middle_value <= 0.0:
                    right_end = middle
                else:
                    left_end = middle
                    left_value = middle_value
            zeros_found.append(0.5 * (left_end + right_end))
        lower = upper
        value_low = value_up
    zeros_found.append(1.0)
    abscissa = [(value + 1.0) / 2.0 for value in zeros_found]
    table_rows = []
    for outer in range(count):
        table_rows.append([0.0] * count)
    for column in range(count):
        factor = [1.0]
        scale = 1.0
        for other in range(count):
            if other != column:
                widened = [0.0] * (len(factor) + 1)
                for power in range(len(factor)):
                    widened[power + 1] = widened[power + 1] + factor[power]
                    widened[power] = widened[power] - abscissa[other] * factor[power]
                factor = widened
                scale = scale * (abscissa[column] - abscissa[other])
        for outer in range(count):
            upto = abscissa[outer]
            accum = 0.0
            for power in range(len(factor)):
                accum = accum + factor[power] * upto ** (power + 1) / (power + 1)
            table_rows[outer][column] = accum / scale
    return (abscissa, table_rows)


def ring_order(count):
    return list(range(0, count, 2)) + list(range(count - 1 - count % 2, 0, -2))


def rows_loop(count, body, most=4):
    step = next(k for k in range(min(most, count), 0, -1) if count % k == 0)

    def some(i, carry):
        for k in range(step):
            body(i * step + k)
        return carry

    lax.fori_loop(0, count // step, some, 0)


def pieces_of(ref):
    return [(z, x) for z in range(ref.shape[1]) for x in range(ref.shape[2])]


def six(ref, row, apart=1):
    deep, wide, tall, lanes = ref.shape[1:]
    here = {at: ref[row, at[0], at[1]] for at in pieces_of(ref)}
    totals = {}
    for z, x in here:
        total = ref[row - 1, z, x] + ref[row + 1, z, x]
        below = here[z - 1, x] if z else pltpu.roll(here[deep - 1, x], 1, 0)
        above = here[z + 1, x] if z < deep - 1 else pltpu.roll(here[0, x], tall - 1, 0)
        if wide == 1:
            left = pltpu.roll(here[z, x], apart, 1)
            right = pltpu.roll(here[z, x], lanes - apart, 1)
        else:
            left = here[z, 1 - x]
            right = pltpu.roll(left, 1 if x == 0 else lanes - 1, 1)
        totals[z, x] = total + (below + above) + (left + right)
    return here, totals


def sweep(src, src_at, source, source_at, dst, dst_at, count, shift, apart=1, most=4):
    weight = OMEGA / (1.0 + 6.0 * shift)
    spread = weight * shift

    def body(row):
        here, totals = six(src, row + src_at, apart)
        for z, x in here:
            dst[row + dst_at, z, x] = (
                (1.0 - OMEGA) * here[z, x] + weight * source[row + source_at, z, x] + spread * totals[z, x]
            )

    rows_loop(count, body, most)


def residual_sums(src, src_at, source, source_at, shift):
    first = six(src, src_at)
    second = six(src, src_at + 1)
    result = []
    for z in range(src.shape[1] // 2):
        forces, heres, sums = [], [], []
        for k, (here, totals) in enumerate((first, second)):
            for at in here:
                if at[0] // 2 == z:
                    forces.append(source[source_at + k, at[0], at[1]])
                    heres.append(here[at])
                    sums.append(totals[at])
        result.append(sum(forces) - (1.0 + 6.0 * shift) * sum(heres) + shift * sum(sums))
    return result


def copy_rows(src, src_at, dst, dst_at, count):
    def body(row):
        for z, x in pieces_of(src):
            dst[row + dst_at, z, x] = src[row + src_at, z, x]

    rows_loop(count, body, 8)


def widen(lo, mid, hi, wide):
    count = mid.shape[0]
    copy_rows(lo, 0, wide, 0, HALO)
    copy_rows(mid, 0, wide, HALO, count)
    copy_rows(hi, 0, wide, HALO + count, HALO)


def lap_and_force(wide, row, kappa):
    here, totals = six(wide, row + 1)
    for z, x in here:
        lap = totals[z, x] - 6.0 * here[z, x]
        value = here[z, x]
        force = DIFFUSE * lap + REACT * kappa[row + 1, z, x] * (value - value * value * value)
        yield (z, x), lap, force


def force_kernel(params, lo, mid, hi, first, kappa, force, base, wide):
    widen(lo, mid, hi, wide)

    def body(row):
        for (z, x), lap, value in lap_and_force(wide, row, kappa):
            force[row, z, x] = value
            base[row, z, x] = first[row + 1, z, x] - params[0] * lap

    rows_loop(force.shape[0], body)


def before(params, wide, right, field, source1, other):
    shift = params[0]
    count = wide.shape[0] - 2 * HALO
    sweep(wide, 1, right, 0, other, 0, count + 6, shift)
    sweep(other, 1, right, 1, field, 0, count + 4, shift)

    def body(row):
        for z, value in enumerate(residual_sums(field, 2 * row + 2, right, 2 * row + 3, shift)):
            source1[row, z, 0] = 0.125 * value

    rows_loop(count // 2, body, 2)


def before_first(params, wide, kappa, field, source1, right, other):
    def body(row):
        for (z, x), lap, force in lap_and_force(wide, row, kappa):
            right[row, z, x] = wide[row + 1, z, x] - params[0] * lap + params[1] * force

    rows_loop(right.shape[0], body)
    before(params, wide, right, field, source1, other)


def before_mixed(count, params, lo, mid, hi, base, *rest):
    forces, (field, source1, right, wide, other) = rest[:count], rest[count:]
    widen(lo, mid, hi, wide)

    def body(row):
        for z, x in pieces_of(base):
            total = base[row, z, x]
            for at, force in enumerate(forces):
                total = total + params[2 + at] * force[row, z, x]
            right[row, z, x] = total

    rows_loop(right.shape[0], body, 2)
    before(params, wide, right, field, source1, other)


def before_again(params, lo, mid, hi, right, field, source1, wide, other):
    widen(lo, mid, hi, wide)
    before(params, wide, right, field, source1, other)


def middle_kernel(params, lo, mid, hi, field1, wide1, source2, first):
    shift = params[0] / 4.0
    count = mid.shape[0]
    widen(lo, mid, hi, wide1)
    weight = OMEGA / (1.0 + 6.0 * shift)

    def start(row):
        for z, x in pieces_of(first):
            first[row, z, x] = weight * wide1[row, z, x]

    rows_loop(count + 2 * HALO, start, 8)
    sweep(first, 1, wide1, 1, field1, 0, count + 6, shift, 1, 11)

    def body(row):
        for z, value in enumerate(residual_sums(field1, 2 * row + 3, wide1, 2 * row + 4, shift)):
            lanes = value.shape[1]
            odd = lax.broadcasted_iota(jnp.int32, value.shape, 1) % 2 == 1
            beside = jnp.where(odd, pltpu.roll(value, 1, 1), pltpu.roll(value, lanes - 1, 1))
            source2[row, z, 0] = 0.125 * (value + beside)

    rows_loop(count // 2, body, 4)


def after_kernel(
    order, params, place, parts, field1, wide1, field, right, out, source2, even, odd, error2, more1, error1, more, last
):
    shift = params[0]
    shift1 = shift / 4.0
    shift2 = shift1 / 4.0
    devices, own = parts.shape[:2]
    rows = devices * own
    weight = OMEGA / (1.0 + 6.0 * shift2)
    for at, device in enumerate(order):
        for row in range(own):
            for z, x in pieces_of(source2):
                value = parts[device, row, z, x]
                source2[at * own + row, z, x] = value
                even[at * own + row + 1, z, x] = weight * value
    here, there = even, odd
    for step in range(COARSE - 1):
        for z, x in pieces_of(here):
            here[0, z, x] = here[rows, z, x]
            here[rows + 1, z, x] = here[1, z, x]
        sweep(here, 1, source2, 0, there, 1, rows, shift2, 2, 16)
        here, there = there, here
    begin = place[0] * own

    def pick(row):
        for z, x in pieces_of(here):
            error2[row, z, x] = here[lax.rem(begin + row - 2 + rows, rows) + 1, z, x]

    rows_loop(own + 4, pick, 12)
    count1 = 2 * own

    def correct1(row):
        for z, x in pieces_of(more1):
            more1[row, z, x] = field1[row, z, x] + error2[(row + 1) // 2, z // 2, x]

    rows_loop(count1 + 6, correct1, 11)
    sweep(more1, 1, wide1, 2, error1, 0, count1 + 4, shift1, 1, 10)
    sweep(error1, 1, wide1, 3, more1, 0, count1 + 2, shift1, 1, 9)
    count = 2 * count1

    def correct(row):
        for z, x in pieces_of(more):
            error = more1[row, z // 2, 0]
            more[2 * row, z, x] = field[2 * row, z, x] + error
            more[2 * row + 1, z, x] = field[2 * row + 1, z, x] + error

    rows_loop(count1 + 2, correct, 3)
    sweep(more, 1, right, 2, last, 0, count + 2, shift)
    sweep(last, 1, right, 3, out, 0, count, shift)


def gather_kernel(devices, part, whole, sends, takes, local):
    me = lax.axis_index("space")
    barrier = pltpu.get_barrier_semaphore()
    for turn in range(1, devices):
        pl.semaphore_signal(
            barrier, inc=1, device_id={"space": lax.rem(me + turn, devices)}, device_id_type=MESH
        )
    pl.semaphore_wait(barrier, devices - 1)
    copies = []
    for turn in range(1, devices):
        copy = pltpu.make_async_remote_copy(
            src_ref=part,
            dst_ref=whole.at[me],
            send_sem=sends.at[turn - 1],
            recv_sem=takes.at[turn - 1],
            device_id={"space": lax.rem(me + turn, devices)},
            device_id_type=MESH,
        )
        copy.start()
        copies.append(copy)
    keep = pltpu.make_async_copy(part, whole.at[me], local)
    keep.start()
    keep.wait()
    for turn, copy in enumerate(copies, 1):
        copy.wait_send()
        came = lax.rem(me - turn + devices, devices)
        pltpu.make_async_remote_copy(
            src_ref=part,
            dst_ref=whole.at[came],
            send_sem=sends.at[turn - 1],
            recv_sem=takes.at[turn - 1],
            device_id={"space": came},
            device_id_type=MESH,
        ).wait_recv()


def ring_sides(devices):
    me = lax.axis_index("space")
    half = (devices + 1) // 2
    rank = jnp.where(me % 2 == 0, me // 2, devices - 1 - me // 2)

    def device(rank):
        return jnp.where(rank < half, 2 * rank, 2 * (devices - 1 - rank) + 1)

    return device(lax.rem(rank + devices - 1, devices)), device(lax.rem(rank + 1, devices))


def halo_kernel(devices, mid, lo, hi, sends, takes):
    before_me, after_me = ring_sides(devices)
    count = mid.shape[0]
    barrier = pltpu.get_barrier_semaphore()
    for side in (before_me, after_me):
        pl.semaphore_signal(barrier, inc=1, device_id={"space": side}, device_id_type=MESH)
    pl.semaphore_wait(barrier, 2)
    copies = []
    for k, (at, dst, side) in enumerate(((count - HALO, lo, after_me), (0, hi, before_me))):
        copy = pltpu.make_async_remote_copy(
            src_ref=mid.at[pl.ds(at, HALO)],
            dst_ref=dst,
            send_sem=sends.at[k],
            recv_sem=takes.at[k],
            device_id={"space": side},
            device_id_type=MESH,
        )
        copy.start()
        copies.append(copy)
    for copy in copies:
        copy.wait()


def call(kernel, outs, scratch, *args, number=None):
    remote = number is not None
    return pl.pallas_call(
        kernel,
        out_shape=[jax.ShapeDtypeStruct(shape, jnp.float32) for shape in outs],
        in_specs=[pl.BlockSpec(memory_space=pltpu.SMEM if a.ndim == 1 else pltpu.VMEM) for a in args],
        out_specs=[pl.BlockSpec(memory_space=pltpu.VMEM)] * len(outs),
        scratch_shapes=[pltpu.VMEM(shape, jnp.float32) if isinstance(shape, tuple) else shape for shape in scratch],
        compiler_params=pltpu.CompilerParams(
            vmem_limit_bytes=60 * 2**20, collective_id=number, has_side_effects=remote
        ),
    )(*args)


def per_device(initial, kappa):
    nodes = lax.axis_size("node")
    position = lax.axis_index("node")
    devices = lax.axis_size("space")
    order = ring_order(devices)
    rank = [order.index(device) for device in range(devices)]
    place = jnp.asarray(rank, jnp.int32)[lax.axis_index("space")][None]
    across = [(i, i ^ 1) for i in range(nodes)]
    abscissa, table_rows = radau_table(nodes)
    table = jnp.asarray(table_rows, jnp.float32)
    shift = jnp.asarray([DIFFUSE * value for value in abscissa], jnp.float32)[position]

    planes, rows, cells = initial.shape
    own = rows // devices
    own1, own2 = own // 2, own // 4
    lanes = cells // 2
    shape0 = (planes, 2, devices, lanes)
    shape1 = (planes // 2, 1, devices, lanes)
    shape2 = (planes // 4, 1, devices, lanes)
    column = jnp.arange(cells)
    unweave = (column[:, None] // 2 + lanes * (column[:, None] % 2) == column[None, :]).astype(jnp.float32)

    def moved(field, matrix):
        return lax.dot_general(
            field, matrix, (((field.ndim - 1,), (0,)), ((), ())), precision=lax.Precision.HIGHEST
        )

    def halo(mid, number):
        lo, hi = call(
            functools.partial(halo_kernel, devices),
            [(HALO,) + mid.shape[1:]] * 2,
            [pltpu.SemaphoreType.DMA((2,))] * 2,
            mid, number=number,
        )
        return lo, mid, hi

    def spread_out(field):
        pieces = moved(field, unweave).reshape(planes, devices, own, cells).transpose(1, 2, 0, 3)
        pieces = jnp.stack([pieces[at] for at in rank])
        pieces = lax.all_to_all(pieces, "space", 0, 0)
        return pieces.reshape(devices, own, planes, 2, lanes).transpose(1, 2, 3, 0, 4)

    def bring_back(field):
        pieces = field.transpose(3, 0, 1, 2, 4).reshape(devices, own, planes, cells)
        pieces = lax.all_to_all(pieces, "space", 0, 0)
        pieces = jnp.stack([pieces[device] for device in order])
        return moved(pieces.transpose(2, 0, 1, 3).reshape(planes, rows, cells), unweave.T)

    first_core = position % 2 == 0
    mine = jnp.concatenate(halo(spread_out(jnp.where(first_core, initial, kappa)), 0))
    others = lax.ppermute(mine, "node", across)
    first = jnp.where(first_core, mine, others)
    strength = jnp.where(first_core, others, mine)

    extra = own + 2 * HALO
    field_outs = [(own + 4,) + shape0, (own1,) + shape1]
    right_out = [(own + 6,) + shape0]
    wide, other = (extra,) + shape0, (own + 6,) + shape0
    params = jnp.stack([shift, jnp.sum(table[position])])
    for step in range(SWEEPS):
        for cycle in range(VCYCLES):
            if cycle:
                field, source1 = call(before_again, field_outs, [wide, other], params, *parts, right)
            elif step == 0:
                field, source1, right = call(
                    before_first, field_outs + right_out, [other], params, first, strength
                )
            else:
                force, base = call(force_kernel, right_out * 2, [wide], params, *parts, first, strength)
                forces, weights = [], []
                for turn in range(nodes // 2):
                    held = force
                    if turn:
                        held = lax.ppermute(force, "node", [(i, (i + 2 * turn) % nodes) for i in range(nodes)])
                    origin = (position - 2 * turn) % nodes
                    forces += [held, lax.ppermute(held, "node", across)]
                    weights += [table[position, origin], table[position, origin ^ 1]]
                field, source1, right = call(
                    functools.partial(before_mixed, nodes),
                    field_outs + right_out, [wide, other],
                    jnp.concatenate([params, jnp.stack(weights)]), *parts, base, *forces,
                )
            field1, wide1, source2 = call(
                middle_kernel,
                [(own1 + 6,) + shape1, (own1 + 8,) + shape1, (own2,) + shape2],
                [(own1 + 8,) + shape1],
                params, *halo(source1, 1),
            )
            (whole,) = call(
                functools.partial(gather_kernel, devices),
                [(devices, own2) + shape2],
                [pltpu.SemaphoreType.DMA((devices - 1,))] * 2 + [pltpu.SemaphoreType.DMA],
                source2, number=2,
            )
            rows2 = own2 * devices
            (section,) = call(
                functools.partial(after_kernel, order),
                [(own,) + shape0],
                [
                    (rows2,) + shape2,
                    (rows2 + 2,) + shape2,
                    (rows2 + 2,) + shape2,
                    (own2 + 4,) + shape2,
                    (own1 + 6,) + shape1,
                    (own1 + 4,) + shape1,
                    (own + 4,) + shape0,
                    (own + 2,) + shape0,
                ],
                params, place, whole, field1, wide1, field, right,
            )
            if step + 1 < SWEEPS or cycle + 1 < VCYCLES:
                parts = halo(section, 0)
    return bring_back(section)[None]


def solution(mesh):
    in_specs = (P("space", None, None), P("space", None, None))
    out_specs = P("node", "space", None, None)
    return jax.shard_map(
        per_device, mesh=mesh, in_specs=in_specs, out_specs=out_specs, check_vma=False
    )
```

```python
import functools

import jax
import jax.numpy as jnp
from jax import lax
from jax.experimental import pallas as pl
from jax.experimental.pallas import tpu as pltpu
from jax.sharding import PartitionSpec as P

SWEEPS = 2
VCYCLES = 2
COARSE = 8

DIFFUSE = 2.0
REACT = 0.5
OMEGA = 0.8

HALO = 4
MESH = pl.DeviceIdType.MESH


def radau_gap(count, where):
    previous = 1.0
    current = where
    for degree in range(1, count):
        following = ((2 * degree + 1) * where * current - degree * previous) / (degree + 1)
        previous = current
        current = following
    return current - previous


def radau_table(count):
    zeros_found = []
    grid_count = 4096
    lower = -1.0
    value_low = radau_gap(count, lower)
    for place in range(1, grid_count):
        upper = -1.0 + 2.0 * place / grid_count
        value_up = radau_gap(count, upper)
        if value_low * value_up < 0.0:
            left_end = lower
            right_end = upper
            left_value = value_low
            for halving in range(100):
                middle = 0.5 * (left_end + right_end)
                middle_value = radau_gap(count, middle)
                if left_value * middle_value <= 0.0:
                    right_end = middle
                else:
                    left_end = middle
                    left_value = middle_value
            zeros_found.append(0.5 * (left_end + right_end))
        lower = upper
        value_low = value_up
    zeros_found.append(1.0)
    abscissa = [(value + 1.0) / 2.0 for value in zeros_found]
    table_rows = []
    for outer in range(count):
        table_rows.append([0.0] * count)
    for column in range(count):
        factor = [1.0]
        scale = 1.0
        for other in range(count):
            if other != column:
                widened = [0.0] * (len(factor) + 1)
                for power in range(len(factor)):
                    widened[power + 1] = widened[power + 1] + factor[power]
                    widened[power] = widened[power] - abscissa[other] * factor[power]
                factor = widened
                scale = scale * (abscissa[column] - abscissa[other])
        for outer in range(count):
            upto = abscissa[outer]
            accum = 0.0
            for power in range(len(factor)):
                accum = accum + factor[power] * upto ** (power + 1) / (power + 1)
            table_rows[outer][column] = accum / scale
    return (abscissa, table_rows)


def ring_order(count):
    return list(range(0, count, 2)) + list(range(count - 1 - count % 2, 0, -2))


def rows_loop(count, body, most=4):
    step = next(k for k in range(min(most, count), 0, -1) if count % k == 0)

    def some(i, carry):
        for k in range(step):
            body(i * step + k)
        return carry

    lax.fori_loop(0, count // step, some, 0)


def pieces_of(ref):
    return [(z, x) for z in range(ref.shape[1]) for x in range(ref.shape[2])]


def six(ref, row, apart=1):
    deep, wide, tall, lanes = ref.shape[1:]
    here = {at: ref[row, at[0], at[1]] for at in pieces_of(ref)}
    totals = {}
    for z, x in here:
        total = ref[row - 1, z, x] + ref[row + 1, z, x]
        below = here[z - 1, x] if z else pltpu.roll(here[deep - 1, x], 1, 0)
        above = here[z + 1, x] if z < deep - 1 else pltpu.roll(here[0, x], tall - 1, 0)
        if wide == 1:
            left = pltpu.roll(here[z, x], apart, 1)
            right = pltpu.roll(here[z, x], lanes - apart, 1)
        else:
            left = here[z, 1 - x]
            right = pltpu.roll(left, 1 if x == 0 else lanes - 1, 1)
        totals[z, x] = total + (below + above) + (left + right)
    return here, totals


def sweep(src, src_at, source, source_at, dst, dst_at, count, shift, apart=1, most=4):
    weight = OMEGA / (1.0 + 6.0 * shift)
    spread = weight * shift

    def body(row):
        here, totals = six(src, row + src_at, apart)
        for z, x in here:
            dst[row + dst_at, z, x] = (
                (1.0 - OMEGA) * here[z, x] + weight * source[row + source_at, z, x] + spread * totals[z, x]
            )

    rows_loop(count, body, most)


def residual_sums(src, src_at, source, source_at, shift):
    first = six(src, src_at)
    second = six(src, src_at + 1)
    result = []
    for z in range(src.shape[1] // 2):
        forces, heres, sums = [], [], []
        for k, (here, totals) in enumerate((first, second)):
            for at in here:
                if at[0] // 2 == z:
                    forces.append(source[source_at + k, at[0], at[1]])
                    heres.append(here[at])
                    sums.append(totals[at])
        result.append(sum(forces) - (1.0 + 6.0 * shift) * sum(heres) + shift * sum(sums))
    return result


def copy_rows(src, src_at, dst, dst_at, count):
    def body(row):
        for z, x in pieces_of(src):
            dst[row + dst_at, z, x] = src[row + src_at, z, x]

    rows_loop(count, body, 8)


def widen(lo, mid, hi, wide):
    count = mid.shape[0]
    copy_rows(lo, 0, wide, 0, HALO)
    copy_rows(mid, 0, wide, HALO, count)
    copy_rows(hi, 0, wide, HALO + count, HALO)


def lap_and_force(wide, row, kappa):
    here, totals = six(wide, row + 1)
    for z, x in here:
        lap = totals[z, x] - 6.0 * here[z, x]
        value = here[z, x]
        force = DIFFUSE * lap + REACT * kappa[row + 1, z, x] * (value - value * value * value)
        yield (z, x), lap, force


def force_kernel(params, lo, mid, hi, first, kappa, force, base, wide):
    widen(lo, mid, hi, wide)

    def body(row):
        for (z, x), lap, value in lap_and_force(wide, row, kappa):
            force[row, z, x] = value
            base[row, z, x] = first[row + 1, z, x] - params[0] * lap

    rows_loop(force.shape[0], body)


def before(params, wide, right, field, source1, other):
    shift = params[0]
    count = wide.shape[0] - 2 * HALO
    sweep(wide, 1, right, 0, other, 0, count + 6, shift)
    sweep(other, 1, right, 1, field, 0, count + 4, shift)

    def body(row):
        for z, value in enumerate(residual_sums(field, 2 * row + 2, right, 2 * row + 3, shift)):
            source1[row, z, 0] = 0.125 * value

    rows_loop(count // 2, body, 2)


def before_first(params, wide, kappa, field, source1, right, other):
    def body(row):
        for (z, x), lap, force in lap_and_force(wide, row, kappa):
            right[row, z, x] = wide[row + 1, z, x] - params[0] * lap + params[1] * force

    rows_loop(right.shape[0], body)
    before(params, wide, right, field, source1, other)


def before_mixed(count, params, lo, mid, hi, base, *rest):
    forces, (field, source1, right, wide, other) = rest[:count], rest[count:]
    widen(lo, mid, hi, wide)

    def body(row):
        for z, x in pieces_of(base):
            total = base[row, z, x]
            for at, force in enumerate(forces):
                total = total + params[2 + at] * force[row, z, x]
            right[row, z, x] = total

    rows_loop(right.shape[0], body, 2)
    before(params, wide, right, field, source1, other)


def before_again(params, lo, mid, hi, right, field, source1, wide, other):
    widen(lo, mid, hi, wide)
    before(params, wide, right, field, source1, other)


def odd_lanes(value):
    return lax.broadcasted_iota(jnp.int32, value.shape, value.ndim - 1) % 2 == 1


def middle(params, lo, mid, hi, field1, wide1, source2, first):
    shift = params[0] / 4.0
    count = mid.shape[0]
    widen(lo, mid, hi, wide1)
    weight = OMEGA / (1.0 + 6.0 * shift)

    def start(row):
        for z, x in pieces_of(first):
            first[row, z, x] = weight * wide1[row, z, x]

    rows_loop(count + 2 * HALO, start, 8)
    sweep(first, 1, wide1, 1, field1, 0, count + 6, shift, 1, 11)

    def body(row):
        evens = residual_sums(field1, 4 * row + 3, wide1, 4 * row + 4, shift)
        odds = residual_sums(field1, 4 * row + 5, wide1, 4 * row + 6, shift)
        for z, (low, high) in enumerate(zip(evens, odds)):
            low = low + pltpu.roll(low, low.shape[1] - 1, 1)
            high = high + pltpu.roll(high, 1, 1)
            source2[row, z, 0] = 0.125 * jnp.where(odd_lanes(low), high, low)

    rows_loop(count // 4, body, 2)


def after(
    order, params, rank, parts, field1, wide1, field, right, out, source2, even, odd, error2, more1, error1, more, last
):
    shift = params[0]
    shift1 = shift / 4.0
    shift2 = shift1 / 4.0
    devices, own = parts.shape[0], 2 * parts.shape[1]
    rows = devices * own
    weight = OMEGA / (1.0 + 6.0 * shift2)
    for at, device in enumerate(order):
        for pair in range(own // 2):
            for z, x in pieces_of(source2):
                value = parts[device, pair, z, x]
                odd_lane = odd_lanes(value)
                low = jnp.where(odd_lane, pltpu.roll(value, 1, 1), value)
                high = jnp.where(odd_lane, value, pltpu.roll(value, value.shape[1] - 1, 1))
                row = at * own + 2 * pair
                source2[row, z, x] = low
                source2[row + 1, z, x] = high
                even[row + 1, z, x] = weight * low
                even[row + 2, z, x] = weight * high
    here, there = even, odd
    for step in range(COARSE - 1):
        for z, x in pieces_of(here):
            here[0, z, x] = here[rows, z, x]
            here[rows + 1, z, x] = here[1, z, x]
        sweep(here, 1, source2, 0, there, 1, rows, shift2, 2, 16)
        here, there = there, here
    begin = rank * own

    def pick(row):
        for z, x in pieces_of(here):
            error2[row, z, x] = here[lax.rem(begin + row - 2 + rows, rows) + 1, z, x]

    rows_loop(own + 4, pick, 12)
    count1 = 2 * own

    def correct1(row):
        for z, x in pieces_of(more1):
            more1[row, z, x] = field1[row, z, x] + error2[(row + 1) // 2, z // 2, x]

    rows_loop(count1 + 6, correct1, 11)
    sweep(more1, 1, wide1, 2, error1, 0, count1 + 4, shift1, 1, 10)
    sweep(error1, 1, wide1, 3, more1, 0, count1 + 2, shift1, 1, 9)
    count = 2 * count1

    def correct(row):
        for z, x in pieces_of(more):
            error = more1[row, z // 2, 0]
            more[2 * row, z, x] = field[2 * row, z, x] + error
            more[2 * row + 1, z, x] = field[2 * row + 1, z, x] + error

    rows_loop(count1 + 2, correct, 3)
    sweep(more, 1, right, 2, last, 0, count + 2, shift)
    sweep(last, 1, right, 3, out, 0, count, shift)


def ring_rank(devices):
    me = lax.axis_index("space")
    return me // 2 + (me % 2) * (devices - 1 - 2 * (me // 2))


def ring_sides(devices):
    half = (devices + 1) // 2
    rank = ring_rank(devices)

    def device(rank):
        return jnp.where(rank < half, 2 * rank, 2 * (devices - 1 - rank) + 1)

    return device(lax.rem(rank + devices - 1, devices)), device(lax.rem(rank + 1, devices))


def halo_kernel(devices, mid, lo, hi, sends, takes):
    before_me, after_me = ring_sides(devices)
    count = mid.shape[0]
    barrier = pltpu.get_barrier_semaphore()
    for side in (before_me, after_me):
        pl.semaphore_signal(barrier, inc=1, device_id={"space": side}, device_id_type=MESH)
    pl.semaphore_wait(barrier, 2)
    copies = []
    for k, (at, dst, side) in enumerate(((count - HALO, lo, after_me), (0, hi, before_me))):
        copy = pltpu.make_async_remote_copy(
            src_ref=mid.at[pl.ds(at, HALO)],
            dst_ref=dst,
            send_sem=sends.at[k],
            recv_sem=takes.at[k],
            device_id={"space": side},
            device_id_type=MESH,
        )
        copy.start()
        copies.append(copy)
    for copy in copies:
        copy.wait()


def halo_copies(mid, lo, hi, sends, takes, sides):
    before_me, after_me = sides
    count = mid.shape[0]
    return [
        pltpu.make_async_remote_copy(
            src_ref=mid.at[pl.ds(at, HALO)],
            dst_ref=dst,
            send_sem=sends.at[k],
            recv_sem=takes.at[k],
            device_id={"space": side},
            device_id_type=MESH,
        )
        for k, (at, dst, side) in enumerate(((count - HALO, lo, after_me), (0, hi, before_me)))
    ]


def cycle_kernel(opening, inputs, order, last_cycle, params, *refs):
    devices = len(order)
    given, refs = refs[:inputs], refs[inputs:]
    makes_right = opening is not before_again
    out, *refs = refs
    lo = hi = None
    if not last_cycle:
        lo, hi, *refs = refs
    if makes_right:
        right, *refs = refs
    else:
        right = given[3]
    (
        wide, other, field, source1, lo1, hi1, field1, wide1, packed, first1, whole,
        source2, even, odd, error2, more1, error1, more, last,
        sends, takes, sends1, takes1, sends2, takes2, local,
    ) = refs
    me = lax.axis_index("space")
    sides = ring_sides(devices)
    barrier = pltpu.get_barrier_semaphore()
    for turn in range(1, devices):
        pl.semaphore_signal(
            barrier, inc=1, device_id={"space": lax.rem(me + turn, devices)}, device_id_type=MESH
        )

    if opening is before_first:
        before_first(params, *given, field, source1, right, other)
    elif opening is before_mixed:
        before_mixed(inputs - 4, params, *given, field, source1, right, wide, other)
    else:
        before_again(params, *given, field, source1, wide, other)

    pl.semaphore_wait(barrier, devices - 1)
    copies = halo_copies(source1, lo1, hi1, sends1, takes1, sides)
    for copy in copies:
        copy.start()
    for copy in copies:
        copy.wait()
    middle(params, lo1, source1, hi1, field1, wide1, packed, first1)

    copies = []
    for turn in range(1, devices):
        copy = pltpu.make_async_remote_copy(
            src_ref=packed,
            dst_ref=whole.at[me],
            send_sem=sends2.at[turn - 1],
            recv_sem=takes2.at[turn - 1],
            device_id={"space": lax.rem(me + turn, devices)},
            device_id_type=MESH,
        )
        copy.start()
        copies.append(copy)
    keep = pltpu.make_async_copy(packed, whole.at[me], local)
    keep.start()
    keep.wait()
    for turn, copy in enumerate(copies, 1):
        copy.wait_send()
        came = lax.rem(me - turn + devices, devices)
        pltpu.make_async_remote_copy(
            src_ref=packed,
            dst_ref=whole.at[came],
            send_sem=sends2.at[turn - 1],
            recv_sem=takes2.at[turn - 1],
            device_id={"space": came},
            device_id_type=MESH,
        ).wait_recv()

    after(
        order, params, ring_rank(devices), whole, field1, wide1, field, right, out,
        source2, even, odd, error2, more1, error1, more, last,
    )
    if not last_cycle:
        copies = halo_copies(out, lo, hi, sends, takes, sides)
        for copy in copies:
            copy.start()
        for copy in copies:
            copy.wait()


def call(kernel, outs, scratch, *args, number=None):
    remote = number is not None
    return pl.pallas_call(
        kernel,
        out_shape=[jax.ShapeDtypeStruct(shape, jnp.float32) for shape in outs],
        in_specs=[pl.BlockSpec(memory_space=pltpu.SMEM if a.ndim == 1 else pltpu.VMEM) for a in args],
        out_specs=[pl.BlockSpec(memory_space=pltpu.VMEM)] * len(outs),
        scratch_shapes=[pltpu.VMEM(shape, jnp.float32) if isinstance(shape, tuple) else shape for shape in scratch],
        compiler_params=pltpu.CompilerParams(
            vmem_limit_bytes=60 * 2**20, collective_id=number, has_side_effects=remote
        ),
    )(*args)


def per_device(initial, kappa):
    nodes = lax.axis_size("node")
    position = lax.axis_index("node")
    devices = lax.axis_size("space")
    order = ring_order(devices)
    rank = [order.index(device) for device in range(devices)]
    place = jnp.asarray(rank, jnp.int32)[lax.axis_index("space")][None]
    across = [(i, i ^ 1) for i in range(nodes)]
    abscissa, table_rows = radau_table(nodes)
    table = jnp.asarray(table_rows, jnp.float32)
    shift = jnp.asarray([DIFFUSE * value for value in abscissa], jnp.float32)[position]

    planes, rows, cells = initial.shape
    own = rows // devices
    own1, own2 = own // 2, own // 4
    lanes = cells // 2
    shape0 = (planes, 2, devices, lanes)
    shape1 = (planes // 2, 1, devices, lanes)
    shape2 = (planes // 4, 1, devices, lanes)
    column = jnp.arange(cells)
    unweave = (column[:, None] // 2 + lanes * (column[:, None] % 2) == column[None, :]).astype(jnp.float32)

    def moved(field, matrix):
        return lax.dot_general(
            field, matrix, (((field.ndim - 1,), (0,)), ((), ())), precision=lax.Precision.HIGHEST
        )

    def halo(mid, number):
        lo, hi = call(
            functools.partial(halo_kernel, devices),
            [(HALO,) + mid.shape[1:]] * 2,
            [pltpu.SemaphoreType.DMA((2,))] * 2,
            mid, number=number,
        )
        return lo, mid, hi

    def spread_out(field):
        pieces = moved(field, unweave).reshape(planes, devices, own, cells).transpose(1, 2, 0, 3)
        pieces = jnp.stack([pieces[at] for at in rank])
        pieces = lax.all_to_all(pieces, "space", 0, 0)
        return pieces.reshape(devices, own, planes, 2, lanes).transpose(1, 2, 3, 0, 4)

    def bring_back(field):
        pieces = field.transpose(3, 0, 1, 2, 4).reshape(devices, own, planes, cells)
        pieces = lax.all_to_all(pieces, "space", 0, 0)
        pieces = jnp.stack([pieces[device] for device in order])
        return moved(pieces.transpose(2, 0, 1, 3).reshape(planes, rows, cells), unweave.T)

    first_core = position % 2 == 0
    mine = jnp.concatenate(halo(spread_out(jnp.where(first_core, initial, kappa)), 0))
    others = lax.ppermute(mine, "node", across)
    first = jnp.where(first_core, mine, others)
    strength = jnp.where(first_core, others, mine)

    extra = own + 2 * HALO
    rows2 = own2 * devices
    right_out = [(own + 6,) + shape0]
    edges = [(HALO,) + shape0] * 2
    dma = pltpu.SemaphoreType.DMA
    scratch = [
        (extra,) + shape0,
        (own + 6,) + shape0,
        (own + 4,) + shape0,
        (own1,) + shape1,
        (HALO,) + shape1,
        (HALO,) + shape1,
        (own1 + 6,) + shape1,
        (own1 + 8,) + shape1,
        (own2 // 2,) + shape2,
        (own1 + 8,) + shape1,
        (devices, own2 // 2) + shape2,
        (rows2,) + shape2,
        (rows2 + 2,) + shape2,
        (rows2 + 2,) + shape2,
        (own2 + 4,) + shape2,
        (own1 + 6,) + shape1,
        (own1 + 4,) + shape1,
        (own + 4,) + shape0,
        (own + 2,) + shape0,
        dma((2,)), dma((2,)), dma((2,)), dma((2,)), dma((devices - 1,)), dma((devices - 1,)), dma,
    ]
    params = jnp.stack([shift, jnp.sum(table[position])])
    for step in range(SWEEPS):
        for cycle in range(VCYCLES):
            scalars = params
            if cycle:
                opening, given = before_again, (*parts, right)
            elif step == 0:
                opening, given = before_first, (first, strength)
            else:
                force, base = call(force_kernel, right_out * 2, [scratch[0]], params, *parts, first, strength)
                forces, weights = [], []
                for turn in range(nodes // 2):
                    held = force
                    if turn:
                        held = lax.ppermute(force, "node", [(i, (i + 2 * turn) % nodes) for i in range(nodes)])
                    origin = (position - 2 * turn) % nodes
                    forces += [held, lax.ppermute(held, "node", across)]
                    weights += [table[position, origin], table[position, origin ^ 1]]
                scalars = jnp.concatenate([params, jnp.stack(weights)])
                opening, given = before_mixed, (*parts, base, *forces)
            last_cycle = step + 1 == SWEEPS and cycle + 1 == VCYCLES
            section, *rest = call(
                functools.partial(cycle_kernel, opening, len(given), order, last_cycle),
                [(own,) + shape0] + ([] if last_cycle else edges) + ([] if cycle else right_out),
                scratch,
                scalars, *given, number=1 + 2 * step + cycle,
            )
            if not last_cycle:
                parts = (rest[0], section, rest[1])
            if not cycle:
                right = rest[-1]
    return bring_back(section)[None]


def solution(mesh):
    in_specs = (P("space", None, None), P("space", None, None))
    out_specs = P("node", "space", None, None)
    return jax.shard_map(
        per_device, mesh=mesh, in_specs=in_specs, out_specs=out_specs, check_vma=False
    )
```

```python
import functools

import jax
import jax.numpy as jnp
from jax import lax
from jax.experimental import pallas as pl
from jax.experimental.pallas import tpu as pltpu
from jax.sharding import PartitionSpec as P

SWEEPS = 2
VCYCLES = 2
COARSE = 8

DIFFUSE = 2.0
REACT = 0.5
OMEGA = 0.8

HALO = 4
MESH = pl.DeviceIdType.MESH


def radau_gap(count, where):
    previous = 1.0
    current = where
    for degree in range(1, count):
        following = ((2 * degree + 1) * where * current - degree * previous) / (degree + 1)
        previous = current
        current = following
    return current - previous


def radau_table(count):
    zeros_found = []
    grid_count = 4096
    lower = -1.0
    value_low = radau_gap(count, lower)
    for place in range(1, grid_count):
        upper = -1.0 + 2.0 * place / grid_count
        value_up = radau_gap(count, upper)
        if value_low * value_up < 0.0:
            left_end = lower
            right_end = upper
            left_value = value_low
            for halving in range(100):
                middle = 0.5 * (left_end + right_end)
                middle_value = radau_gap(count, middle)
                if left_value * middle_value <= 0.0:
                    right_end = middle
                else:
                    left_end = middle
                    left_value = middle_value
            zeros_found.append(0.5 * (left_end + right_end))
        lower = upper
        value_low = value_up
    zeros_found.append(1.0)
    abscissa = [(value + 1.0) / 2.0 for value in zeros_found]
    table_rows = []
    for outer in range(count):
        table_rows.append([0.0] * count)
    for column in range(count):
        factor = [1.0]
        scale = 1.0
        for other in range(count):
            if other != column:
                widened = [0.0] * (len(factor) + 1)
                for power in range(len(factor)):
                    widened[power + 1] = widened[power + 1] + factor[power]
                    widened[power] = widened[power] - abscissa[other] * factor[power]
                factor = widened
                scale = scale * (abscissa[column] - abscissa[other])
        for outer in range(count):
            upto = abscissa[outer]
            accum = 0.0
            for power in range(len(factor)):
                accum = accum + factor[power] * upto ** (power + 1) / (power + 1)
            table_rows[outer][column] = accum / scale
    return (abscissa, table_rows)


def ring_order(count):
    return list(range(0, count, 2)) + list(range(count - 1 - count % 2, 0, -2))


def rows_loop(count, body, most=4):
    step = next(k for k in range(min(most, count), 0, -1) if count % k == 0)

    def some(i, carry):
        for k in range(step):
            body(i * step + k)
        return carry

    lax.fori_loop(0, count // step, some, 0)


def pieces_of(ref):
    return [(z, x) for z in range(ref.shape[1]) for x in range(ref.shape[2])]


def six(ref, row, apart=1):
    deep, wide, tall, lanes = ref.shape[1:]
    here = {at: ref[row, at[0], at[1]] for at in pieces_of(ref)}
    totals = {}
    for z, x in here:
        total = ref[row - 1, z, x] + ref[row + 1, z, x]
        below = here[z - 1, x] if z else pltpu.roll(here[deep - 1, x], 1, 0)
        above = here[z + 1, x] if z < deep - 1 else pltpu.roll(here[0, x], tall - 1, 0)
        if wide == 1:
            left = pltpu.roll(here[z, x], apart, 1)
            right = pltpu.roll(here[z, x], lanes - apart, 1)
        else:
            left = here[z, 1 - x]
            right = pltpu.roll(left, 1 if x == 0 else lanes - 1, 1)
        totals[z, x] = total + (below + above) + (left + right)
    return here, totals


def sweep(src, src_at, source, source_at, dst, dst_at, count, shift, apart=1, most=4):
    weight = OMEGA / (1.0 + 6.0 * shift)
    spread = weight * shift

    def body(row):
        here, totals = six(src, row + src_at, apart)
        for z, x in here:
            dst[row + dst_at, z, x] = (
                (1.0 - OMEGA) * here[z, x] + weight * source[row + source_at, z, x] + spread * totals[z, x]
            )

    rows_loop(count, body, most)


def residual_sums(src, src_at, source, source_at, shift):
    first = six(src, src_at)
    second = six(src, src_at + 1)
    result = []
    for z in range(src.shape[1] // 2):
        forces, heres, sums = [], [], []
        for k, (here, totals) in enumerate((first, second)):
            for at in here:
                if at[0] // 2 == z:
                    forces.append(source[source_at + k, at[0], at[1]])
                    heres.append(here[at])
                    sums.append(totals[at])
        result.append(sum(forces) - (1.0 + 6.0 * shift) * sum(heres) + shift * sum(sums))
    return result


def copy_rows(src, src_at, dst, dst_at, count):
    def body(row):
        for z, x in pieces_of(src):
            dst[row + dst_at, z, x] = src[row + src_at, z, x]

    rows_loop(count, body, 8)


def widen(lo, mid, hi, wide):
    count = mid.shape[0]
    copy_rows(lo, 0, wide, 0, HALO)
    copy_rows(mid, 0, wide, HALO, count)
    copy_rows(hi, 0, wide, HALO + count, HALO)


def lap_and_force(wide, row, kappa):
    here, totals = six(wide, row + 1)
    for z, x in here:
        lap = totals[z, x] - 6.0 * here[z, x]
        value = here[z, x]
        force = DIFFUSE * lap + REACT * kappa[row + 1, z, x] * (value - value * value * value)
        yield (z, x), lap, force


def force_kernel(params, lo, mid, hi, first, kappa, force, base, wide):
    widen(lo, mid, hi, wide)

    def body(row):
        for (z, x), lap, value in lap_and_force(wide, row, kappa):
            force[row, z, x] = value
            base[row, z, x] = first[row + 1, z, x] - params[0] * lap

    rows_loop(force.shape[0], body)


def before(params, wide, right, field, source1, other):
    shift = params[0]
    count = wide.shape[0] - 2 * HALO
    sweep(wide, 1, right, 0, other, 0, count + 6, shift)
    sweep(other, 1, right, 1, field, 0, count + 4, shift)

    def body(row):
        for z, value in enumerate(residual_sums(field, 2 * row + 2, right, 2 * row + 3, shift)):
            source1[row, z, 0] = 0.125 * value

    rows_loop(count // 2, body, 2)


def before_first(params, wide, kappa, field, source1, right, other):
    def body(row):
        for (z, x), lap, force in lap_and_force(wide, row, kappa):
            right[row, z, x] = wide[row + 1, z, x] - params[0] * lap + params[1] * force

    rows_loop(right.shape[0], body)
    before(params, wide, right, field, source1, other)


def before_mixed(count, params, lo, mid, hi, base, *rest):
    forces, (field, source1, right, wide, other) = rest[:count], rest[count:]
    widen(lo, mid, hi, wide)

    def body(row):
        for z, x in pieces_of(base):
            total = base[row, z, x]
            for at, force in enumerate(forces):
                total = total + params[2 + at] * force[row, z, x]
            right[row, z, x] = total

    rows_loop(right.shape[0], body, 2)
    before(params, wide, right, field, source1, other)


def before_again(params, lo, mid, hi, right, field, source1, wide, other):
    widen(lo, mid, hi, wide)
    before(params, wide, right, field, source1, other)


def odd_lanes(value):
    return lax.broadcasted_iota(jnp.int32, value.shape, value.ndim - 1) % 2 == 1


def middle(params, lo, mid, hi, field1, wide1, source2, first):
    shift = params[0] / 4.0
    count = mid.shape[0]
    widen(lo, mid, hi, wide1)
    weight = OMEGA / (1.0 + 6.0 * shift)

    def start(row):
        for z, x in pieces_of(first):
            first[row, z, x] = weight * wide1[row, z, x]

    rows_loop(count + 2 * HALO, start, 8)
    sweep(first, 1, wide1, 1, field1, 0, count + 6, shift, 1, 11)

    def body(row):
        evens = residual_sums(field1, 4 * row + 3, wide1, 4 * row + 4, shift)
        odds = residual_sums(field1, 4 * row + 5, wide1, 4 * row + 6, shift)
        for z, (low, high) in enumerate(zip(evens, odds)):
            low = low + pltpu.roll(low, low.shape[1] - 1, 1)
            high = high + pltpu.roll(high, 1, 1)
            source2[row, z, 0] = 0.125 * jnp.where(odd_lanes(low), high, low)

    rows_loop(count // 4, body, 2)


def after(
    order, params, rank, parts, field1, wide1, field, right, out, source2, even, odd, error2, more1, error1, more, last
):
    shift = params[0]
    shift1 = shift / 4.0
    shift2 = shift1 / 4.0
    devices, own = parts.shape[0], 2 * parts.shape[1]
    rows = devices * own
    weight = OMEGA / (1.0 + 6.0 * shift2)
    for at, device in enumerate(order):
        for pair in range(own // 2):
            for z, x in pieces_of(source2):
                value = parts[device, pair, z, x]
                odd_lane = odd_lanes(value)
                low = jnp.where(odd_lane, pltpu.roll(value, 1, 1), value)
                high = jnp.where(odd_lane, value, pltpu.roll(value, value.shape[1] - 1, 1))
                row = at * own + 2 * pair
                source2[row, z, x] = low
                source2[row + 1, z, x] = high
                even[row + 1, z, x] = weight * low
                even[row + 2, z, x] = weight * high
    here, there = even, odd
    for step in range(COARSE - 1):
        for z, x in pieces_of(here):
            here[0, z, x] = here[rows, z, x]
            here[rows + 1, z, x] = here[1, z, x]
        sweep(here, 1, source2, 0, there, 1, rows, shift2, 2, 16)
        here, there = there, here
    begin = rank * own

    def pick(row):
        for z, x in pieces_of(here):
            error2[row, z, x] = here[lax.rem(begin + row - 2 + rows, rows) + 1, z, x]

    rows_loop(own + 4, pick, 12)
    count1 = 2 * own

    def correct1(row):
        for z, x in pieces_of(more1):
            more1[row, z, x] = field1[row, z, x] + error2[(row + 1) // 2, z // 2, x]

    rows_loop(count1 + 6, correct1, 11)
    sweep(more1, 1, wide1, 2, error1, 0, count1 + 4, shift1, 1, 10)
    sweep(error1, 1, wide1, 3, more1, 0, count1 + 2, shift1, 1, 9)
    count = 2 * count1

    def correct(row):
        for z, x in pieces_of(more):
            error = more1[row, z // 2, 0]
            more[2 * row, z, x] = field[2 * row, z, x] + error
            more[2 * row + 1, z, x] = field[2 * row + 1, z, x] + error

    rows_loop(count1 + 2, correct, 3)
    sweep(more, 1, right, 2, last, 0, count + 2, shift)
    sweep(last, 1, right, 3, out, 0, count, shift)


def ring_rank(devices):
    me = lax.axis_index("space")
    return me // 2 + (me % 2) * (devices - 1 - 2 * (me // 2))


def ring_sides(devices):
    half = (devices + 1) // 2
    rank = ring_rank(devices)

    def device(rank):
        return jnp.where(rank < half, 2 * rank, 2 * (devices - 1 - rank) + 1)

    return device(lax.rem(rank + devices - 1, devices)), device(lax.rem(rank + 1, devices))


def halo_kernel(devices, mid, lo, hi, sends, takes):
    before_me, after_me = ring_sides(devices)
    count = mid.shape[0]
    barrier = pltpu.get_barrier_semaphore()
    for side in (before_me, after_me):
        pl.semaphore_signal(barrier, inc=1, device_id={"space": side}, device_id_type=MESH)
    pl.semaphore_wait(barrier, 2)
    copies = []
    for k, (at, dst, side) in enumerate(((count - HALO, lo, after_me), (0, hi, before_me))):
        copy = pltpu.make_async_remote_copy(
            src_ref=mid.at[pl.ds(at, HALO)],
            dst_ref=dst,
            send_sem=sends.at[k],
            recv_sem=takes.at[k],
            device_id={"space": side},
            device_id_type=MESH,
        )
        copy.start()
        copies.append(copy)
    for copy in copies:
        copy.wait()


def halo_copies(mid, lo, hi, sends, takes, sides):
    before_me, after_me = sides
    count = mid.shape[0]
    return [
        pltpu.make_async_remote_copy(
            src_ref=mid.at[pl.ds(at, HALO)],
            dst_ref=dst,
            send_sem=sends.at[k],
            recv_sem=takes.at[k],
            device_id={"space": side},
            device_id_type=MESH,
        )
        for k, (at, dst, side) in enumerate(((count - HALO, lo, after_me), (0, hi, before_me)))
    ]


def cycle_kernel(opening, inputs, order, last_cycle, params, *refs):
    devices = len(order)
    given, refs = refs[:inputs], refs[inputs:]
    makes_right = opening is not before_again
    out, *refs = refs
    lo = hi = None
    if not last_cycle:
        lo, hi, *refs = refs
    if makes_right:
        right, *refs = refs
    else:
        right = given[3]
    (
        wide, other, field, source1, lo1, hi1, field1, wide1, packed, first1, whole,
        source2, even, odd, error2, more1, error1, more, last,
        sends, takes, sends1, takes1, sends2, takes2, local,
    ) = refs
    me = lax.axis_index("space")
    sides = ring_sides(devices)
    barrier = pltpu.get_barrier_semaphore()
    for turn in range(1, devices):
        pl.semaphore_signal(
            barrier, inc=1, device_id={"space": lax.rem(me + turn, devices)}, device_id_type=MESH
        )

    if opening is before_first:
        before_first(params, *given, field, source1, right, other)
    elif opening is before_mixed:
        before_mixed(inputs - 4, params, *given, field, source1, right, wide, other)
    else:
        before_again(params, *given, field, source1, wide, other)

    pl.semaphore_wait(barrier, devices - 1)
    copies = halo_copies(source1, lo1, hi1, sends1, takes1, sides)
    for copy in copies:
        copy.start()
    for copy in copies:
        copy.wait()
    middle(params, lo1, source1, hi1, field1, wide1, packed, first1)

    copies = []
    for turn in range(1, devices):
        copy = pltpu.make_async_remote_copy(
            src_ref=packed,
            dst_ref=whole.at[me],
            send_sem=sends2.at[turn - 1],
            recv_sem=takes2.at[turn - 1],
            device_id={"space": lax.rem(me + turn, devices)},
            device_id_type=MESH,
        )
        copy.start()
        copies.append(copy)
    keep = pltpu.make_async_copy(packed, whole.at[me], local)
    keep.start()
    keep.wait()
    for turn, copy in enumerate(copies, 1):
        copy.wait_send()
        came = lax.rem(me - turn + devices, devices)
        pltpu.make_async_remote_copy(
            src_ref=packed,
            dst_ref=whole.at[came],
            send_sem=sends2.at[turn - 1],
            recv_sem=takes2.at[turn - 1],
            device_id={"space": came},
            device_id_type=MESH,
        ).wait_recv()

    after(
        order, params, ring_rank(devices), whole, field1, wide1, field, right, out,
        source2, even, odd, error2, more1, error1, more, last,
    )
    if not last_cycle:
        copies = halo_copies(out, lo, hi, sends, takes, sides)
        for copy in copies:
            copy.start()
        for copy in copies:
            copy.wait()


def call(kernel, outs, scratch, *args, number=None):
    remote = number is not None
    return pl.pallas_call(
        kernel,
        out_shape=[jax.ShapeDtypeStruct(shape, jnp.float32) for shape in outs],
        in_specs=[pl.BlockSpec(memory_space=pltpu.SMEM if a.ndim == 1 else pltpu.VMEM) for a in args],
        out_specs=[pl.BlockSpec(memory_space=pltpu.VMEM)] * len(outs),
        scratch_shapes=[pltpu.VMEM(shape, jnp.float32) if isinstance(shape, tuple) else shape for shape in scratch],
        compiler_params=pltpu.CompilerParams(
            vmem_limit_bytes=60 * 2**20, collective_id=number, has_side_effects=remote
        ),
    )(*args)


def per_device(initial, kappa):
    nodes = lax.axis_size("node")
    position = lax.axis_index("node")
    devices = lax.axis_size("space")
    order = ring_order(devices)
    rank = [order.index(device) for device in range(devices)]
    across = [(i, i ^ 1) for i in range(nodes)]
    abscissa, table_rows = radau_table(nodes)
    scalars = []
    for node in range(nodes):
        weights = table_rows[node]
        turned = [weights[((node - 2 * turn) % nodes) ^ side] for turn in range(nodes // 2) for side in range(2)]
        scalars.append([DIFFUSE * abscissa[node], sum(weights)] + turned)
    params = lax.dynamic_index_in_dim(jnp.asarray(scalars, jnp.float32), position, 0, False)

    planes, rows, cells = initial.shape
    own = rows // devices
    own1, own2 = own // 2, own // 4
    lanes = cells // 2
    shape0 = (planes, 2, devices, lanes)
    shape1 = (planes // 2, 1, devices, lanes)
    shape2 = (planes // 4, 1, devices, lanes)
    column = jnp.arange(cells)
    unweave = (column[:, None] // 2 + lanes * (column[:, None] % 2) == column[None, :]).astype(jnp.float32)

    def moved(field, matrix):
        return lax.dot_general(
            field, matrix, (((field.ndim - 1,), (0,)), ((), ())), precision=lax.Precision.HIGHEST
        )

    def halo(mid, number):
        lo, hi = call(
            functools.partial(halo_kernel, devices),
            [(HALO,) + mid.shape[1:]] * 2,
            [pltpu.SemaphoreType.DMA((2,))] * 2,
            mid, number=number,
        )
        return lo, mid, hi

    def spread_out(field):
        pieces = moved(field, unweave).reshape(planes, devices, own, cells).transpose(1, 2, 0, 3)
        pieces = jnp.stack([pieces[at] for at in rank])
        pieces = lax.all_to_all(pieces, "space", 0, 0)
        return pieces.reshape(devices, own, planes, 2, lanes).transpose(1, 2, 3, 0, 4)

    def bring_back(field):
        pieces = field.transpose(3, 0, 1, 2, 4).reshape(devices, own, planes, cells)
        pieces = lax.all_to_all(pieces, "space", 0, 0)
        pieces = jnp.stack([pieces[device] for device in order])
        return moved(pieces.transpose(2, 0, 1, 3).reshape(planes, rows, cells), unweave.T)

    first_core = position % 2 == 0
    mine = jnp.concatenate(halo(spread_out(jnp.where(first_core, initial, kappa)), 0))
    others = lax.ppermute(mine, "node", across)
    first = jnp.where(first_core, mine, others)
    strength = jnp.where(first_core, others, mine)

    extra = own + 2 * HALO
    rows2 = own2 * devices
    right_out = [(own + 6,) + shape0]
    edges = [(HALO,) + shape0] * 2
    dma = pltpu.SemaphoreType.DMA
    scratch = [
        (extra,) + shape0,
        (own + 6,) + shape0,
        (own + 4,) + shape0,
        (own1,) + shape1,
        (HALO,) + shape1,
        (HALO,) + shape1,
        (own1 + 6,) + shape1,
        (own1 + 8,) + shape1,
        (own2 // 2,) + shape2,
        (own1 + 8,) + shape1,
        (devices, own2 // 2) + shape2,
        (rows2,) + shape2,
        (rows2 + 2,) + shape2,
        (rows2 + 2,) + shape2,
        (own2 + 4,) + shape2,
        (own1 + 6,) + shape1,
        (own1 + 4,) + shape1,
        (own + 4,) + shape0,
        (own + 2,) + shape0,
        dma((2,)), dma((2,)), dma((2,)), dma((2,)), dma((devices - 1,)), dma((devices - 1,)), dma,
    ]
    for step in range(SWEEPS):
        for cycle in range(VCYCLES):
            if cycle:
                opening, given = before_again, (*parts, right)
            elif step == 0:
                opening, given = before_first, (first, strength)
            else:
                force, base = call(force_kernel, right_out * 2, [scratch[0]], params, *parts, first, strength)
                forces = []
                for turn in range(nodes // 2):
                    held = force
                    if turn:
                        held = lax.ppermute(force, "node", [(i, (i + 2 * turn) % nodes) for i in range(nodes)])
                    forces += [held, lax.ppermute(held, "node", across)]
                opening, given = before_mixed, (*parts, base, *forces)
            last_cycle = step + 1 == SWEEPS and cycle + 1 == VCYCLES
            section, *rest = call(
                functools.partial(cycle_kernel, opening, len(given), order, last_cycle),
                [(own,) + shape0] + ([] if last_cycle else edges) + ([] if cycle else right_out),
                scratch,
                params, *given, number=1 + 2 * step + cycle,
            )
            if not last_cycle:
                parts = (rest[0], section, rest[1])
            if not cycle:
                right = rest[-1]
    return bring_back(section)[None]


def solution(mesh):
    in_specs = (P("space", None, None), P("space", None, None))
    out_specs = P("node", "space", None, None)
    return jax.shard_map(
        per_device, mesh=mesh, in_specs=in_specs, out_specs=out_specs, check_vma=False
    )
```
